32 devices in a mesh: tp: 8 (over z, y), ep: 4 (over x, core).
Axes of the slice: x: 2, y: 2, z: 4, core: 2. Of those that a mesh axis runs over, the one named last changes fastest.
Arguments:
- x: bfloat16 [16384, 2048], P(('ep', 'tp'))
- idx: int32 [16384, 4], P(('ep', 'tp'))
- g: float32 [16384, 4], P(('ep', 'tp'))
- slot: int32 [16384, 4], P(('ep', 'tp'))
- ws1: bfloat16 [2048, 5632], P(None, 'tp')
- ws3: bfloat16 [2048, 5632], P(None, 'tp')
- ws2: bfloat16 [5632, 2048], P('tp')
- w1: bfloat16 [60, 2048, 1408], P('ep')
- w3: bfloat16 [60, 2048, 1408], P('ep')
- w2: bfloat16 [60, 1408, 2048], P('ep')
Outputs:
- output: bfloat16 [16384, 2048], P(('ep', 'tp'))
All inputs are finite; a program needn't handle non-finite values.
Results may differ from the reference program's by a relative error of at most 0.001.
Values are sent between devices in bfloat16 or wider.
A program may use at most 1.25 GiB of HBM per device.

```python
import jax
import jax.numpy as jnp
from jax import lax

D = 2048
F = 1408
FS = 5632
E = 60
K = 4
TOK = 512
DEV = 32
C = 72

T = TOK * DEV
ROWS = DEV * C


def _weights(key, n, shape, fan_in):
    return lax.map(lambda kk: (jax.random.normal(kk, shape, jnp.float32) * fan_in ** -0.5).astype(jnp.bfloat16), jax.random.split(key, n))


def _positions(idx):
    oh = jax.nn.one_hot(idx.reshape(DEV, TOK * K), E, dtype=jnp.int32)
    return jnp.sum((jnp.cumsum(oh, axis=1) - 1) * oh, axis=-1).reshape(T, K)


def _route_ids(key):
    weight = jnp.uint32(96) + (jnp.uint32(256) * jnp.arange(E, dtype=jnp.uint32)) // jnp.uint32(E)
    wait = (jax.random.bits(key, (T, E), jnp.uint32) >> 10) * weight[None, :]
    return jnp.argsort(wait, axis=-1, stable=True)[:, :K].astype(jnp.int32)


def setup_inputs(seed: int = 0) -> dict:
    ks = jax.random.split(jax.random.PRNGKey(seed), 10)
    x = jax.random.normal(ks[0], (T, D), jnp.float32).astype(jnp.bfloat16)
    idx = _route_ids(jax.random.fold_in(ks[1], 7))
    g = jax.random.uniform(ks[2], (T, K), jnp.float32, 0.4, 1.0)
    pos = _positions(idx)
    slot = jnp.where(pos < C, C - 1 - pos, -1).astype(jnp.int32)
    return {
        "x": x, "idx": idx, "g": g, "slot": slot,
        "ws1": _weights(ks[3], 1, (D, FS), D)[0],
        "ws3": _weights(ks[4], 1, (D, FS), D)[0],
        "ws2": _weights(ks[5], 1, (FS, D), FS)[0],
        "w1": _weights(ks[6], E, (D, F), D),
        "w3": _weights(ks[7], E, (D, F), D),
        "w2": _weights(ks[8], E, (F, D), F),
    }


def _swiglu(x, w1, w3, w2):
    a = jnp.dot(x, w1, preferred_element_type=jnp.float32)
    b = jnp.dot(x, w3, preferred_element_type=jnp.float32)
    h = (jax.nn.silu(a) * b).astype(jnp.bfloat16)
    return jnp.dot(h, w2, preferred_element_type=jnp.float32)


def reference(x, idx, g, slot, ws1, ws3, ws2, w1, w3, w2):
    s = _swiglu(x, ws1, ws3, ws2)
    blk = (jnp.arange(T, dtype=jnp.int32) // TOK)[:, None]
    kept = slot >= 0
    dest = jnp.where(kept, idx * ROWS + blk * C + slot, E * ROWS)
    buf = jnp.zeros((E * ROWS, D), jnp.bfloat16)
    for j in range(K):
        buf = buf.at[dest[:, j]].set(x, mode="drop")
    out = lax.map(lambda a: _swiglu(*a).astype(jnp.bfloat16), (buf.reshape(E, ROWS, D), w1, w3, w2))
    out = out.reshape(E * ROWS, D)
    gate = jnp.where(kept, g, 0.0)
    src = jnp.where(kept, dest, 0)
    y = x.astype(jnp.float32) + s
    for j in range(K):
        y = y + gate[:, j:j + 1] * jnp.take(out, src[:, j], axis=0).astype(jnp.float32)
    return y.astype(jnp.bfloat16)
```

```python
import functools

import jax
import jax.numpy as jnp
from jax import lax
from jax.experimental import pallas as pl
from jax.experimental.pallas import tpu as pltpu
from jax.sharding import PartitionSpec as P


F32, BF16, I32 = jnp.float32, jnp.bfloat16, jnp.int32
D = 2048
TOK = 512
EL = 15
F = 1408
CAP = 72
MP = 4 * CAP
EG = 3
SUB = 176
GRP = 384
DB = 1024
LT = DB // 128
PITCH = LT + 1
ACC = (TOK + 1) * LT

CORE = [(0, 1), (1, 0), (2, 3), (3, 2)]
XSW = [(0, 2), (1, 3), (2, 0), (3, 1)]
YSW = [(p, p ^ 1) for p in range(8)]

HBM = pl.BlockSpec(memory_space=pl.ANY)


def _params(vmem=60, **more):
    return pltpu.CompilerParams(vmem_limit_bytes=vmem << 20, **more)


def _cost(flops, nbytes):
    return pl.CostEstimate(flops=int(flops), bytes_accessed=int(nbytes), transcendentals=0)


def _silu_mul(a, b):
    return a * jax.nn.sigmoid(a) * b


def _copy(src, dst, sem):
    return pltpu.make_async_copy(src, dst, sem)


RING = 5


def _front_kernel(x, meta, w13, wq2, w1, w3, h, hs, w2a, w2b, lists,
                  xv, mv, wv, lhs, hv, wg, sv, bounce,
                  xsem, msem, wsem, hsem, ssem, lsem, bsem, xsend, xrecv, msend, mrecv, wsend, wrecv, asend, arecv, csend, crecv):
    tp, q = lax.axis_index("tp"), lax.axis_index("ep")
    z = tp // 2
    mid = (z == 1) | (z == 2)
    end = (z == 0) | (z == 3)
    near = {"ep": q + 1 - 2 * lax.rem(q, 2)}
    far = {"ep": lax.rem(q + 2, 4)}
    other = {"tp": tp + 1 - 2 * lax.rem(tp, 2)}
    pair = {"tp": tp + 2 - 4 * lax.rem(z, 2)}
    across = {"tp": lax.rem(tp, 2) + 2 * (3 - z)}

    barrier = pltpu.get_barrier_semaphore()
    for d in (near, far, other, pair):
        pl.semaphore_signal(barrier, inc=1, device_id=d, device_id_type=pl.DeviceIdType.MESH)
    pl.when(mid)(lambda: pl.semaphore_signal(barrier, inc=1, device_id=across, device_id_type=pl.DeviceIdType.MESH))
    pl.semaphore_wait(barrier, 4 + z * (3 - z) // 2)

    def remote(src, dst, send, recv, device):
        return pltpu.make_async_remote_copy(src_ref=src, dst_ref=dst, send_sem=send, recv_sem=recv, device_id=device,
                                            device_id_type=pl.DeviceIdType.MESH)

    m_near = remote(meta, mv.at[1], msend.at[0], mrecv.at[1], near)
    m_far = remote(meta, mv.at[2], msend.at[1], mrecv.at[2], far)
    m_cross = remote(mv.at[2], mv.at[3], msend.at[2], mrecv.at[3], near)
    x_near = remote(x, xv.at[1], xsend.at[0], xrecv.at[1], near)
    x_far = remote(x, xv.at[2], xsend.at[1], xrecv.at[2], far)
    x_cross = remote(xv.at[2], xv.at[3], xsend.at[2], xrecv.at[3], near)
    x_own = _copy(x, xv.at[0], xsem.at[0])
    m_own = _copy(meta, mv.at[0], msem.at[0])

    def up(src, slot, n, device):
        return remote(src, wg.at[slot], wsend.at[n], wrecv.at[slot], device)

    u_y = [up(w13 if k == 0 else wg.at[2 * k], 2 * k + 1, k, other) for k in range(4)]
    u_pair = {0: up(w13, 2, 4, pair), 2: up(wg.at[4], 4, 5, pair), 3: up(wg.at[6], 6, 6, pair)}
    u_mid = {0: up(w13, 4, 7, across), 1: up(wg.at[2], 6, 8, across)}
    u_own = _copy(w13, wg.at[0], lsem.at[0])

    def down(src, slot, n, device):
        return remote(src, w2a.at[slot], asend.at[n], arecv.at[slot], device)

    def later(src, slot, n, device):
        return remote(src, w2b.at[slot], csend.at[n], crecv.at[slot], device)

    wa, wb = wq2.at[0], wq2.at[1]
    a_y = [down(wa if k == 0 else w2a.at[2 * k], 2 * k + 1, k, other) for k in range(4)]
    a_pair = {0: down(wa, 2, 4, pair), 2: down(w2a.at[4], 4, 5, pair), 3: down(w2a.at[6], 6, 6, pair)}
    a_mid = {0: down(wa, 4, 7, across), 1: down(w2a.at[2], 6, 8, across)}
    c_pair = {0: later(wb, 1, 0, pair), 2: later(w2b.at[2], 2, 1, pair), 3: later(w2b.at[3], 3, 2, pair)}
    c_mid = {0: later(wb, 2, 3, across), 1: later(w2b.at[1], 3, 4, across)}
    got = lambda c: c.wait_recv()

    for c in (m_near, m_far, x_near, x_far, u_y[0], u_pair[0]):
        c.start()
    pl.when(mid)(u_mid[0].start)

    @pl.when(end)
    def _():
        a_pair[0].start()
        c_pair[0].start()

    for c in (m_own, x_own, u_own):
        c.start()

    def weights(m):
        slot, e = lax.rem(m, RING), m // 2

        def either(what):
            pl.when(lax.rem(m, 2) == 0)(lambda: what(_copy(w1.at[e], wv.at[slot], wsem.at[slot])))
            pl.when(lax.rem(m, 2) == 1)(lambda: what(_copy(w3.at[e], wv.at[slot], wsem.at[slot])))

        return either

    for m in range(RING):
        weights(m)(lambda c: c.start())
    b_in, b_out = _copy(wb, bounce, bsem.at[0]), _copy(bounce, w2b.at[0], bsem.at[1])
    b_in.start()
    m_own.wait()
    x_own.wait()
    got(m_far)
    m_cross.start()
    got(m_near)
    got(m_cross)
    b_in.wait()
    b_out.start()

    got(u_pair[0])
    u_y[1].start()

    @pl.when(mid)
    def _():
        u_mid[1].start()
        got(u_mid[0])
        u_pair[2].start()
        u_y[2].start()

    got(x_near)
    got(x_far)
    x_cross.start()
    got(x_cross)

    def second():
        @pl.when(end)
        def _():
            got(u_pair[2])
            u_y[2].start()

        @pl.when(mid)
        def _():
            got(u_mid[1])
            u_pair[3].start()
            u_y[3].start()
            a_mid[0].start()
            a_pair[0].start()
            got(a_pair[0])
            a_mid[1].start()
            c_mid[0].start()
            c_pair[0].start()
            got(c_pair[0])
            c_mid[1].start()

    def third():
        @pl.when(end)
        def _():
            got(u_pair[3])
            u_y[3].start()
            a_y[0].start()

        @pl.when(mid)
        def _():
            a_y[0].start()
            a_y[1].start()
            got(a_mid[0])
            a_pair[2].start()
            a_y[2].start()
            got(a_mid[1])
            a_pair[3].start()
            a_y[3].start()
            got(c_mid[0])
            c_pair[2].start()
            got(c_mid[1])
            c_pair[3].start()

    def fourth():
        @pl.when(end)
        def _():
            for k, c in ((1, a_pair[0]), (2, a_pair[2]), (3, a_pair[3])):
                got(c)
                a_y[k].start()

    rows = EG * CAP
    row = lax.broadcasted_iota(I32, (rows, TOK), 0).astype(F32)
    tok = lax.broadcasted_iota(I32, (rows, TOK), 1).astype(F32) - float(TOK)
    lane = lax.broadcasted_iota(I32, (rows, 128), 1)

    def group(k, carry):
        first = (q * EL * CAP + k * rows).astype(F32)
        at = pl.ds(pl.multiple_of(k * rows, 8), rows)

        def half(p, cols):
            hots = []
            for j in range(2):
                s = 2 * p + j
                gate = jnp.zeros((rows, TOK), F32)
                for i in range(4):
                    gate = gate + jnp.where(mv[s, i:i + 1, :] - first == row, mv[s, 4 + i:5 + i, :], 0.0)
                hit = gate > 0.0
                hots.append(jnp.where(hit, 1.0, 0.0).astype(BF16))
                t = jnp.sum(jnp.where(hit, tok, 0.0), axis=1, keepdims=True) + float(TOK)
                gt = jnp.sum(gate, axis=1, keepdims=True)
                cols = jnp.where(lane == s, t, jnp.where(lane == 4 + s, gt, cols))
            to = pl.ds(pl.multiple_of(p * 2 * CAP, 16), 2 * CAP)
            for n in range(0, D, 256):
                r = [jnp.dot(hots[j], xv[2 * p + j, :, n:n + 256], preferred_element_type=F32) for j in range(2)]
                for e in range(EG):
                    lhs[e, to, n:n + 256] = jnp.concatenate(
                        [r[0][e * CAP:(e + 1) * CAP], r[1][e * CAP:(e + 1) * CAP]], axis=0).astype(BF16)
            return cols

        lists[at, :] = lax.fori_loop(0, 2, half, jnp.zeros((rows, 128), F32))

        def expert(e3, carry):
            e = k * EG + e3
            slot0, slot1, out = lax.rem(2 * e, RING), lax.rem(2 * e + 1, RING), lax.rem(e, 2)
            weights(2 * e)(lambda c: c.wait())
            weights(2 * e + 1)(lambda c: c.wait())
            pl.when(e >= 2)(lambda: _copy(hv.at[out], h.at[e - 2], hsem.at[out]).wait())
            a = lhs[e3]
            for n in range(0, F, 128):
                w = jnp.concatenate([wv[slot0, :, n:n + 128], wv[slot1, :, n:n + 128]], axis=1)
                r = jnp.dot(a, w, preferred_element_type=F32)
                hv[out, :, n:n + 128] = _silu_mul(r[:, :128], r[:, 128:]).astype(BF16)
            _copy(hv.at[out], h.at[e], hsem.at[out]).start()
            for m in range(2):
                pl.when(2 * e + RING + m < 2 * EL)(lambda m=m: weights(2 * e + RING + m)(lambda c: c.start()))
            return carry

        lax.fori_loop(0, EG, expert, 0)
        pl.when(k == 0)(second)
        pl.when(k == 2)(third)
        return carry

    lax.fori_loop(0, EL // EG, group, 0)
    fourth()

    half = TOK // 2
    u_own.wait()

    def block(j, carry):
        k, i = j // 8, lax.rem(j, 8)
        for kk in range(4):
            pl.when(j == 8 * kk)(lambda kk=kk: got(u_y[kk]))
        slot = lax.rem(j, 2)
        pl.when(j >= 2)(lambda: _copy(sv.at[slot], hs.at[0, pl.ds(0, half)], ssem.at[slot]).wait())
        a = xv[i // 2, pl.ds(pl.multiple_of(lax.rem(i, 2) * half, half), half), :]
        pad = jnp.zeros((GRP - 2 * SUB, D), BF16)
        w = jnp.concatenate([wg[2 * k, :SUB, :], wg[2 * k + 1, :SUB, :], pad, wg[2 * k, SUB:, :], wg[2 * k + 1, SUB:, :], pad], axis=0)
        r = lax.dot_general(a, w, (((1,), (1,)), ((), ())), preferred_element_type=F32)
        sv[slot] = _silu_mul(r[:, :GRP], r[:, GRP:]).astype(BF16)
        _copy(sv.at[slot], hs.at[k, pl.ds(pl.multiple_of(i * half, half), half)], ssem.at[slot]).start()
        return carry

    lax.fori_loop(0, 32, block, 0)

    for slot in range(2):
        _copy(sv.at[slot], hs.at[0, pl.ds(0, half)], ssem.at[slot]).wait()
        _copy(hv.at[slot], h.at[0], hsem.at[slot]).wait()
    for c in a_y:
        got(c)

    @pl.when(end)
    def _():
        for c in (c_pair[0], c_pair[2], c_pair[3]):
            got(c)

    b_out.wait()
    for c in [m_near, m_far, m_cross, x_near, x_far, x_cross] + u_y + a_y + [u_pair[0], a_pair[0], c_pair[0]]:
        c.wait_send()

    @pl.when(mid)
    def _():
        for c in (u_mid[0], u_mid[1], u_pair[2], u_pair[3], a_mid[0], a_mid[1], a_pair[2], a_pair[3],
                  c_mid[0], c_mid[1], c_pair[2], c_pair[3]):
            c.wait_send()


def _front(x, meta, w13, wq2, w1, w3):
    dma = pltpu.SemaphoreType.DMA
    vmem = pltpu.VMEM
    return pl.pallas_call(
        _front_kernel,
        in_specs=[HBM] * 6,
        out_specs=[HBM] * 4 + [pl.BlockSpec(memory_space=pltpu.VMEM)],
        out_shape=[jax.ShapeDtypeStruct((EL, MP, F), BF16), jax.ShapeDtypeStruct((4, 4 * TOK, GRP), BF16),
                   jax.ShapeDtypeStruct((8, SUB, DB), BF16), jax.ShapeDtypeStruct((4, SUB, DB), BF16),
                   jax.ShapeDtypeStruct((EL * CAP, 128), F32)],
        scratch_shapes=[vmem((4, TOK, D), BF16), vmem((4, 8, TOK), F32), vmem((RING, D, F), BF16), vmem((EG, MP, D), BF16),
                        vmem((2, MP, F), BF16), vmem((8, 2 * SUB, D), BF16), vmem((2, TOK // 2, GRP), BF16), vmem((SUB, DB), BF16),
                        dma((1,)), dma((1,)), dma((RING,)), dma((2,)), dma((2,)), dma((1,)), dma((2,)),
                        dma((3,)), dma((4,)), dma((3,)), dma((4,)), dma((9,)), dma((8,)), dma((9,)), dma((8,)), dma((5,)), dma((4,))],
        compiler_params=_params(collective_id=1, has_side_effects=True),
        cost_estimate=_cost(EL * 2 * MP * D * 2 * F + 2 * 4 * TOK * D * 8 * GRP, EL * 4 * D * F),
        name="front",
    )(x, meta, w13, wq2, w1, w3)


WRING = 8
HRING = 6


def _down_kernel(c, tok, gate, hs, w_own, *rest):
    ws, (h, w2, own, near, far, cross), scratch = rest[:2 - (c == 0)], rest[2 - (c == 0):8 - (c == 0)], rest[8 - (c == 0):]
    sv, wsq, acc, res, wv, hv, ssem, qsem, wsem, hsem, osem = scratch
    rows = TOK // 2
    cols = pl.ds(c * DB, DB)

    def weights(k):
        slot = lax.rem(k, WRING)
        return _copy(w2.at[k, :, cols], wv.at[slot], wsem.at[slot])

    def hidden(k):
        slot = lax.rem(k, HRING)
        return _copy(h.at[k], hv.at[slot], hsem.at[slot])

    loads = []
    for k in range(4):
        for j in range(2):
            if k == 0 and j == 0:
                src = w_own.at[c]
            else:
                src = ws[0].at[2 * k + j] if c == 0 else ws[j].at[k]
            loads.append(_copy(src, wsq.at[pl.ds(k * GRP + j * SUB, SUB)], qsem.at[2 * k + j]))
    halves = []
    for b in range(2):
        at = pl.ds(b * 2 * TOK, 2 * TOK)
        halves.append([_copy(hs.at[k, at], sv.at[k, at], ssem.at[b, k]) for k in range(4)])
    for x in loads + halves[0] + halves[1]:
        x.start()
    for k in range(WRING):
        weights(k).start()
    for k in range(HRING):
        hidden(k).start()
    for k in range(4):
        wsq[k * GRP + 2 * SUB:(k + 1) * GRP, :] = jnp.zeros((GRP - 2 * SUB, DB), BF16)
    for x in loads:
        x.wait()

    def shared(i, carry):
        at = pl.ds(pl.multiple_of(i * rows, rows), rows)
        a = jnp.concatenate([sv[k, at, :] for k in range(4)], axis=1)
        base = pl.multiple_of(i // 2 * ACC + lax.rem(i, 2) * (rows * LT), 8)
        for n in range(0, DB, 256):
            r = jnp.dot(a, wsq[:, n:n + 256], preferred_element_type=F32)
            for j in range(2):
                for b in range(rows // 8):
                    acc[pl.ds(base + b * 8 * LT + n // 128 + j, 8, stride=LT), :] = r[8 * b:8 * b + 8, 128 * j:128 * j + 128]
        return carry

    for b in range(2):
        for x in halves[b]:
            x.wait()
        lax.fori_loop(4 * b, 4 * b + 4, shared, 0)

    def expert(e, carry):
        weights(e).wait()
        hidden(e).wait()
        wslot, hslot = lax.rem(e, WRING), lax.rem(e, HRING)
        a = hv[hslot]
        for n in range(0, DB, 256):
            r = jnp.dot(a, wv[wslot, :, n:n + 256], preferred_element_type=F32).astype(BF16).astype(F32)
            for j in range(2):
                for b in range(MP // 8):
                    res[pl.ds(b * 8 * PITCH + n // 128 + j, 8, stride=PITCH), :] = r[8 * b:8 * b + 8, 128 * j:128 * j + 128]

        @pl.when(e + WRING < EL)
        def _():
            weights(e + WRING).start()

        @pl.when(e + HRING < EL)
        def _():
            hidden(e + HRING).start()

        for s in range(4):
            def step(k, carry, s=s):
                new = []
                for u in range(8):
                    j = ((e * CAP + k * 8 + u) * 4) + s
                    t = pl.multiple_of(s * ACC + tok[j] * LT, LT)
                    row = res[pl.ds((s * CAP + k * 8 + u) * PITCH, LT), :]
                    new.append((t, acc[pl.ds(t, LT), :] + gate[j] * row))
                for t, v in new:
                    acc[pl.ds(t, LT), :] = v
                return carry

            lax.fori_loop(0, CAP // 8, step, 0)
        return carry

    lax.fori_loop(0, EL, expert, 0)
    outs = [_copy(acc.at[pl.ds(k * ACC, ACC)], o, osem.at[k]) for k, o in ((3, cross), (2, far), (1, near), (0, own))]
    for x in outs:
        x.start()
    for x in outs:
        x.wait()


def _down(c, tok, gate, hs, w_own, ws, h, w2):
    dma = pltpu.SemaphoreType.DMA
    return pl.pallas_call(
        functools.partial(_down_kernel, c),
        grid_spec=pltpu.PrefetchScalarGridSpec(
            num_scalar_prefetch=2,
            grid=(1,),
            in_specs=[HBM] * (4 + len(ws)),
            out_specs=[HBM] * 4,
            scratch_shapes=[pltpu.VMEM((4, 4 * TOK, GRP), BF16), pltpu.VMEM((4 * GRP, DB), BF16), pltpu.VMEM((4 * ACC, 128), F32),
                            pltpu.VMEM((MP * PITCH, 128), F32), pltpu.VMEM((WRING, F, DB), BF16), pltpu.VMEM((HRING, MP, F), BF16),
                            dma((2, 4)), dma((8,)), dma((WRING,)), dma((HRING,)), dma((4,))],
        ),
        out_shape=[jax.ShapeDtypeStruct((ACC, 128), F32)] * 4,
        compiler_params=_params(),
        cost_estimate=_cost(2 * 4 * TOK * 4 * GRP * DB + EL * 2 * MP * F * DB, EL * 2 * F * DB),
        name="down",
    )(tok, gate, hs, w_own, *ws, h, w2)


FR = 128


def _final_kernel(c, x, own, near, far, *rest):
    y, xv, tv, yv, xsem, tsem, ysem = rest[-7:]
    cols = pl.ds(c * DB, DB)
    n = TOK // FR

    def loads(k):
        at = pl.ds(k * FR * LT, FR * LT)
        return [_copy(x.at[pl.ds(k * FR, FR), cols], xv.at[k], xsem.at[k])] + [
            _copy(t.at[at], tv.at[k, j], tsem.at[k, j]) for j, t in enumerate((own, near, far))]

    def store(k):
        return _copy(yv.at[k], y.at[pl.ds(k * FR, FR), cols], ysem.at[k])

    for k in range(n):
        for m in loads(k):
            m.start()

    for k in range(n):
        for m in loads(k):
            m.wait()
        for b in range(FR // 8):
            for l in range(LT):
                at = pl.ds(b * 8 * LT + l, 8, stride=LT)
                v = tv[k, 0, at, :] + tv[k, 1, at, :] + tv[k, 2, at, :]
                lanes = slice(l * 128, l * 128 + 128)
                yv[k, 8 * b:8 * b + 8, lanes] = (xv[k, 8 * b:8 * b + 8, lanes].astype(F32) + v).astype(BF16)
        store(k).start()
    for k in range(n):
        store(k).wait()


def _final(c, x, terms, y):
    n = TOK // FR
    dma = pltpu.SemaphoreType.DMA
    extra = [] if y is None else [y]
    return pl.pallas_call(
        functools.partial(_final_kernel, c),
        in_specs=[HBM] * (4 + len(extra)),
        out_specs=HBM,
        out_shape=jax.ShapeDtypeStruct((TOK, D), BF16),
        scratch_shapes=[pltpu.VMEM((n, FR, DB), BF16), pltpu.VMEM((n, 3, FR * LT, 128), F32), pltpu.VMEM((n, FR, DB), BF16),
                        dma((n,)), dma((n, 3)), dma((n,))],
        input_output_aliases={4: 0} if extra else {},
        compiler_params=_params(),
        cost_estimate=_cost(TOK * DB * 256, 16 * TOK * DB),
        name="final",
    )(x, *terms, *extra)


def solution(mesh):
    rows = P(("ep", "tp"), None)

    def layer(x, idx, g, slot, ws1, ws3, ws2, w1, w3, w2):
        sub = lax.axis_index("ep") * SUB
        key = jnp.where(slot >= 0, idx * CAP + slot, -1)
        meta = jnp.concatenate([key.astype(F32).T, g.T], axis=0)
        w13 = jnp.concatenate([lax.dynamic_slice(w, (0, sub), (D, SUB)).T for w in (ws1, ws3)], axis=0)
        wq2 = lax.dynamic_slice(ws2, (sub, 0), (SUB, D))
        wq2 = jnp.stack([wq2[:, c * DB:(c + 1) * DB] for c in range(D // DB)])
        h, hs, w2a, w2b, lists = _front(x, meta, w13, wq2, w1, w3)
        w2o = lax.ppermute(w2b, "tp", YSW)
        tok = lists[:, :4].astype(I32).reshape(-1)
        gate = lists[:, 4:8].reshape(-1)

        y = None
        for c in range(D // DB):
            own, near, far, cross = _down(c, tok, gate, hs, wq2, (w2a,) if c == 0 else (w2b, w2o), h, w2)
            cross = lax.ppermute(cross, "ep", CORE)
            near = lax.ppermute(near, "ep", CORE)
            far = lax.ppermute(far + cross, "ep", XSW)
            y = _final(c, x, (own, near, far), y)
        return y

    return jax.shard_map(
        layer, mesh=mesh,
        in_specs=(rows, rows, rows, rows, P(None, "tp"), P(None, "tp"), P("tp", None),
                  P("ep", None, None), P("ep", None, None), P("ep", None, None)),
        out_specs=rows, check_vma=False)
```
